32 devices in a mesh: grp: 8 (over z, core), dom: 4 (over y, x).
Axes of the slice: x: 2, y: 2, z: 4, core: 2. Of those that a mesh axis runs over, the one named last changes fastest.
Arguments:
- connect: int32 [20, 4096], P(None, ('grp', 'dom')), may hold values from 0 to 511, as said below
- interface_nodes: int32 [32, 4, 32], P(('grp', 'dom')), may hold values from 0 to 511, as said below
- neighbours: int32 [32, 4], P(('grp', 'dom')), may hold values from 0 to 1, as said below
- point_rank: int32 [32, 2048], P(('grp', 'dom')), may hold values from 0 to 2047, each once within a row
- shape_grad: float32 [48, 20], replicated, may hold values from -1.25 to 1.25
- inverse_jacobian: float32 [9, 4096], P(None, ('grp', 'dom')), may hold values from -0.45 to 2.5
- lame_moduli: float32 [2, 4096], P(None, ('grp', 'dom')), may hold values from 0.5 to 2
- point_weights: float32 [16, 4096], P(None, ('grp', 'dom')), may hold values from 0.003 to 0.02
- mass_elem: float32 [20, 4096], P(None, ('grp', 'dom')), may hold values from 0.5 to 2
- source_pattern: float32 [3, 16384], P(None, ('grp', 'dom')), may hold values from -6 to 6
- wavelet: float32 [16], replicated, may hold values from -6 to 6
Outputs:
- strain_db: bfloat16 [16, 6, 65536], P(None, None, ('grp', 'dom'))
The draws below stay inside these ranges and needn't reach their ends.
Inputs may be any that keep to these rules, and one draw needn't show every extreme that they name: `connect`: every one of a partition's 512 nodes is named by some element of that partition. `interface_nodes`: entry i of list k of a partition and entry i of the opposite list of the partition beside it in direction k are copies of one node; no node stands twice among a partition's four lists. `neighbours`: the entry of a partition in direction k equals that of the partition beside it in the opposite direction; it is 0 where no partition lies in direction k.
All inputs are finite; a program needn't handle non-finite values.
Results may differ from the reference program's by a relative error of at most 0.001.
Values may be sent and summed in bfloat16 or wider, within the bound.
A program may use at most 64 MiB of HBM per device.

```python
import math
import jax
import jax.numpy as jnp
from jax import lax

ELEM_DEV = 128
EL_NODES = 20
POINTS = 16
STRAIN = 6
STEPS = 16
NODE_DEV = 512
FACE_NODES = 32
PT_DEV = 2048
GROUPS = 8
WRITERS = 4
PARTS_SIZE = 32
ELEMS = 4096
NODES = 16384


def draw_connect(key, part):
    streams = jax.random.split(key, PARTS_SIZE)

    def one_partition(stream):
        first_key, second_key = jax.random.split(stream)
        shuffled = jax.random.permutation(first_key, EL_NODES * ELEM_DEV)
        filler = jax.random.randint(second_key, (EL_NODES * ELEM_DEV,), 0, NODE_DEV)
        node_ids = jnp.where(shuffled < NODE_DEV, shuffled, filler)
        return node_ids.reshape(EL_NODES, ELEM_DEV).astype(jnp.int32)
    blocks = jax.vmap(one_partition)(streams)
    return blocks.transpose(1, 0, 2).reshape(EL_NODES, PARTS_SIZE * ELEM_DEV)


def draw_interface_nodes(key, part):
    streams = jax.random.split(jax.random.fold_in(key, 11), PARTS_SIZE)

    def pick_lists(stream):
        shuffled = jax.random.permutation(stream, NODE_DEV)
        return shuffled[:4 * FACE_NODES].reshape(4, FACE_NODES).astype(jnp.int32)
    return jax.vmap(pick_lists)(streams)


def draw_neighbours(key, part):
    first_key, second_key = jax.random.split(jax.random.fold_in(key, 23))
    vertical = (jax.random.randint(first_key, (GROUPS, WRITERS), 0, 4) < 3).astype(jnp.int32)
    vertical = vertical * (jnp.arange(GROUPS) < GROUPS - 1).astype(jnp.int32)[:, None]
    lateral = (jax.random.randint(second_key, (GROUPS, WRITERS), 0, 4) < 3).astype(jnp.int32)
    lateral = lateral * (jnp.arange(WRITERS) < WRITERS - 1).astype(jnp.int32)[None, :]
    toward_lower = jnp.concatenate([jnp.zeros((1, WRITERS), jnp.int32), vertical[:-1]], axis=0)
    toward_left = jnp.concatenate([jnp.zeros((GROUPS, 1), jnp.int32), lateral[:, :-1]], axis=1)
    table = jnp.stack([toward_lower, vertical, toward_left, lateral], axis=2)
    return table.reshape(PARTS_SIZE, 4).astype(jnp.int32)


def draw_inverse_jacobian(key, part):
    first_key, second_key = jax.random.split(jax.random.fold_in(key, 37))
    count = PARTS_SIZE * ELEM_DEV
    diagonal = jnp.exp(jax.random.uniform(first_key, (3, count), jnp.float32, -0.5, 0.5))
    shearing = jnp.clip(0.25 * jax.random.normal(second_key, (3, 3, count), jnp.float32), -0.45, 0.45)
    identity = jnp.eye(3, dtype=jnp.float32)
    matrix = shearing * (1.0 - identity)[:, :, None] + identity[:, :, None] * diagonal[:, None, :]
    return matrix.reshape(9, count).astype(jnp.float32)


def level_of(stream_key, extent, shards, smallest, top_value):
    def one(position, shards_of):
        steps = jax.random.uniform(jax.random.fold_in(jax.random.fold_in(stream_key, 6), position), (shards_of,), jnp.float32, smallest / len(shards), top_value / len(shards))
        return jnp.repeat(jnp.exp(steps), extent[position] // shards_of).reshape((-1,) + (1,) * (len(extent) - position - 1))

    gain = one(*shards[0])
    for cut in shards[1:]:
        gain = gain * one(*cut)
    return gain


def gaussian(rng, dims, spread, bound, pieces=(), kind=jnp.bfloat16):
    loudness = level_of(rng, dims, pieces, -0.22, 0.18) if pieces else 1.0
    values = jax.random.normal(rng, dims, jnp.float32) * spread * loudness
    return jnp.minimum(jnp.maximum(values, -bound), bound).astype(kind)


def setup_inputs(seed: int = 0) -> dict:
    arg_keys = jax.random.split(jax.random.key(seed), 12)
    return {
        "connect": draw_connect(jax.random.fold_in(arg_keys[11], 71), 0),
        "interface_nodes": draw_interface_nodes(jax.random.fold_in(arg_keys[11], 71), 0),
        "neighbours": draw_neighbours(jax.random.fold_in(arg_keys[11], 71), 0),
        "point_rank": jax.vmap(lambda own: jax.random.permutation(own, PT_DEV))(jax.random.split(arg_keys[3], PARTS_SIZE)).reshape((PARTS_SIZE, PT_DEV)).astype(jnp.int32),
        "shape_grad": gaussian(arg_keys[4], (3 * POINTS, EL_NODES), EL_NODES ** -0.5, 1.25, (), jnp.float32),
        "inverse_jacobian": draw_inverse_jacobian(jax.random.fold_in(arg_keys[11], 71), 0),
        "lame_moduli": jnp.clip(jnp.exp(math.log(2.0) - 1.3862944 * jax.random.uniform(arg_keys[6], (2, ELEMS), jnp.float32) ** level_of(arg_keys[6], (2, ELEMS), ((1, 32),), -0.2, 0.2)), 0.5, 2.0),
        "point_weights": jnp.clip(jnp.exp(math.log(0.02) - 1.89712 * jax.random.uniform(arg_keys[7], (POINTS, ELEMS), jnp.float32) ** level_of(arg_keys[7], (POINTS, ELEMS), ((1, 32),), -0.2, 0.2)), 0.003, 0.02),
        "mass_elem": jnp.clip(jnp.exp(math.log(2.0) - 1.3862944 * jax.random.uniform(arg_keys[8], (EL_NODES, ELEMS), jnp.float32) ** level_of(arg_keys[8], (EL_NODES, ELEMS), ((1, 32),), -0.2, 0.2)), 0.5, 2.0),
        "source_pattern": gaussian(arg_keys[9], (3, NODES), 1.0, 6.0, ((1, 32),), jnp.float32),
        "wavelet": gaussian(arg_keys[10], (STEPS,), 1.0, 6.0, (), jnp.float32),
    }


time_step = 0.5


def gradient_at(displace, connect, shape_grad, inverse_jacobian):
    elements = connect.shape[1]
    node_values = jnp.take(displace, connect, axis=1)
    along_ref = jnp.einsum('mn,cne->cme', shape_grad, node_values, precision=lax.Precision.HIGHEST)
    along_ref = along_ref.reshape(3, 3, POINTS, elements)
    jacobian = inverse_jacobian.reshape(3, 3, elements)
    result = along_ref[:, 0, None] * jacobian[0][None, :, None, :]
    result = result + along_ref[:, 1, None] * jacobian[1][None, :, None, :]
    result = result + along_ref[:, 2, None] * jacobian[2][None, :, None, :]
    return result


def strain_of(tensor):
    return jnp.stack([tensor[0, 0], tensor[1, 1], tensor[2, 2],
                      0.5 * (tensor[1, 2] + tensor[2, 1]),
                      0.5 * (tensor[0, 2] + tensor[2, 0]),
                      0.5 * (tensor[0, 1] + tensor[1, 0])], axis=0)


def element_forces(tensor, lame_moduli, point_weights, inverse_jacobian, shape_grad, connect, node_count):
    elements = connect.shape[1]
    jacobian = inverse_jacobian.reshape(3, 3, elements)
    volume_change = tensor[0, 0] + tensor[1, 1] + tensor[2, 2]
    identity = jnp.eye(3, dtype=jnp.float32)
    stress = lame_moduli[1][None, None, None, :] * (tensor + tensor.transpose(1, 0, 2, 3))
    stress = stress + identity[:, :, None, None] * (lame_moduli[0][None, :] * volume_change)[None, None]
    mapped = stress[:, 0][:, None] * jacobian[:, 0][None, :, None, :]
    mapped = mapped + stress[:, 1][:, None] * jacobian[:, 1][None, :, None, :]
    mapped = mapped + stress[:, 2][:, None] * jacobian[:, 2][None, :, None, :]
    mapped = mapped * point_weights[None, None]
    node_values = jnp.einsum('mn,cme->cne', shape_grad, mapped.reshape(3, 3 * POINTS, elements),
                             precision=lax.Precision.HIGHEST)
    return jnp.zeros((3, node_count), jnp.float32).at[:, connect].add(node_values)


def split_parts(array, width):
    return array.reshape(array.shape[0], PARTS_SIZE, width).transpose(1, 0, 2)


def assemble_parts(node_field, interface_nodes, neighbours):
    channels = node_field.shape[1]
    picked = jax.vmap(lambda values, shared: jnp.take(values, shared, axis=1))(node_field, interface_nodes)
    picked = picked.reshape(GROUPS, WRITERS, channels, 4, FACE_NODES)
    zero_row = jnp.zeros((1, WRITERS, channels, FACE_NODES), jnp.float32)
    zero_column = jnp.zeros((GROUPS, 1, channels, FACE_NODES), jnp.float32)
    from_below = jnp.concatenate([zero_row, picked[:-1, :, :, 1]], axis=0)
    from_above = jnp.concatenate([picked[1:, :, :, 0], zero_row], axis=0)
    from_left = jnp.concatenate([zero_column, picked[:, :-1, :, 3]], axis=1)
    from_right = jnp.concatenate([picked[:, 1:, :, 2], zero_column], axis=1)
    received = jnp.stack([from_below, from_above, from_left, from_right], axis=3)
    received = received.reshape(PARTS_SIZE, channels, 4, FACE_NODES)
    received = received * neighbours.astype(jnp.float32)[:, None, :, None]
    return jax.vmap(lambda values, shared, incoming: values.at[:, shared].add(incoming))(
        node_field, interface_nodes, received)


def reference(connect, interface_nodes, neighbours, point_rank, shape_grad, inverse_jacobian,
              lame_moduli, point_weights, mass_elem, source_pattern, wavelet):
    connect_parts = split_parts(connect, ELEM_DEV)
    jacobian_parts = split_parts(inverse_jacobian, ELEM_DEV)
    moduli_parts = split_parts(lame_moduli, ELEM_DEV)
    weight_parts = split_parts(point_weights, ELEM_DEV)
    mass_parts = split_parts(mass_elem, ELEM_DEV)
    pattern_parts = split_parts(source_pattern, NODE_DEV)
    node_mass = jax.vmap(lambda connect_part, mass_part: jnp.zeros((1, NODE_DEV), jnp.float32).at[0, connect_part].add(mass_part))(connect_parts, mass_parts)
    inverse_mass = 1.0 / assemble_parts(node_mass, interface_nodes, neighbours)
    gradient_all = jax.vmap(gradient_at, in_axes=(0, 0, None, 0))
    forces_all = jax.vmap(lambda tensor, moduli, weight_part, jacobian_part, connect_part: element_forces(
        tensor, moduli, weight_part, jacobian_part, shape_grad, connect_part, NODE_DEV))

    def advance(loop_state, wave):
        displace, velocity = loop_state
        tensor = gradient_all(displace, connect_parts, shape_grad, jacobian_parts)
        force = wave * pattern_parts - forces_all(tensor, moduli_parts, weight_parts, jacobian_parts, connect_parts)
        force = assemble_parts(force, interface_nodes, neighbours)
        velocity = velocity + time_step * inverse_mass * force
        displace = displace + time_step * velocity
        snapshot = jax.vmap(strain_of)(gradient_all(displace, connect_parts, shape_grad, jacobian_parts))
        snapshot = snapshot.reshape(PARTS_SIZE, STRAIN, PT_DEV).astype(jnp.bfloat16)
        return (displace, velocity), snapshot

    start = jnp.zeros((PARTS_SIZE, 3, NODE_DEV), jnp.float32)
    unused, snapshots = lax.scan(advance, (start, start), wavelet)
    inverse_rank = jax.vmap(lambda ranking: jnp.zeros((PT_DEV,), jnp.int32).at[ranking].set(
        jnp.arange(PT_DEV, dtype=jnp.int32)))(point_rank)
    ordered = jax.vmap(lambda values, positions: jnp.take(values, positions, axis=2),
                       in_axes=(1, 0), out_axes=1)(snapshots, inverse_rank)
    per_writer = PT_DEV // WRITERS
    ordered = ordered.reshape(STEPS, GROUPS, WRITERS, STRAIN, WRITERS, per_writer).transpose(0, 3, 1, 4, 2, 5)
    return ordered.reshape(STEPS, STRAIN, PARTS_SIZE * PT_DEV)
```

```python
import functools

import jax
import jax.numpy as jnp
from jax import lax
from jax.experimental import pallas as pl
from jax.experimental.pallas import tpu as pltpu
from jax.sharding import PartitionSpec as P

MESH = pl.DeviceIdType.MESH
F32 = jnp.float32
BF16 = jnp.bfloat16
time_step = 0.5
LANES = 128


def split(x):
    hi = x.astype(BF16)
    return hi, (x - hi.astype(F32)).astype(BF16)


def pick_lanes(x, idx):
    return jnp.take_along_axis(x, idx, axis=1, mode="promise_in_bounds")


def kernel(
    groups,
    writers,
    steps,
    nodes_el,
    conn_ref,
    connt_ref,
    facet_ref,
    facesw_ref,
    nb_ref,
    rankt_ref,
    w1f_ref,
    w2f_ref,
    jac_ref,
    lame_ref,
    pw_ref,
    mass_ref,
    src_ref,
    wav_ref,
    out_ref,
    onehot,
    hmask,
    perm,
    w1,
    w2,
    snaps,
    lhs,
    ordered,
    send,
    recv,
    send_sem,
    recv_sem,
    out_send_sem,
    out_recv_sem,
):
    g = lax.axis_index("grp")
    d = lax.axis_index("dom")
    points = pw_ref.shape[0]
    block = out_ref.shape[2] // writers
    blocks = src_ref.shape[1] // LANES

    recv[...] = jnp.zeros_like(recv)
    has = (g > 0, g < groups - 1, d > 0, d < writers - 1)
    where_to = ((g - 1, d), (g + 1, d), (g, d - 1), (g, d + 1))

    barrier = pltpu.get_barrier_semaphore()
    for k in range(2):

        @pl.when(has[k])
        def _():
            pl.semaphore_signal(barrier, inc=1, device_id=where_to[k], device_id_type=MESH)

    for i in range(1, writers):
        pl.semaphore_signal(
            barrier, inc=1, device_id=(g, lax.rem(d + i, writers)), device_id_type=MESH
        )

    lane128 = lax.broadcasted_iota(jnp.int32, (LANES, LANES), 1)
    row16 = lax.broadcasted_iota(jnp.int32, (16, LANES), 0)
    for n in range(nodes_el):
        low = jnp.bitwise_and(connt_ref[:, n : n + 1], LANES - 1)
        onehot[n * LANES : (n + 1) * LANES, :] = jnp.where(low == lane128, 1.0, 0.0).astype(BF16)
        high = jnp.right_shift(conn_ref[n : n + 1, :], 7)
        hmask[n * 16 : (n + 1) * 16, :] = jnp.where(
            high == jnp.right_shift(row16, 2), 1.0, 0.0
        ).astype(BF16)
    for ref, full in ((w1, w1f_ref), (w2, w2f_ref)):
        hi, lo = split(full[...])
        col = lax.broadcasted_iota(jnp.int32, full.shape, 1)
        ref[...] = jnp.where(
            col < (full.shape[1] // 3) * 2, hi.astype(F32), lo.astype(F32)
        ).astype(BF16)

    facesw = facesw_ref[...]
    face_low = jnp.broadcast_to(jnp.bitwise_and(facesw, LANES - 1), (8, LANES))
    face_mask = jnp.where(
        jnp.right_shift(facesw, 7) == jnp.right_shift(row16, 2), 1.0, 0.0
    )
    position = lax.broadcasted_iota(jnp.int32, (LANES, LANES), 0).astype(F32)
    inv_rows = []
    has_rows = []
    for b in range(blocks):
        hit = jnp.where(facet_ref[...] == lane128 + b * LANES, 1.0, 0.0)
        inv_rows.append(
            jnp.broadcast_to(jnp.sum(hit * position, axis=0, keepdims=True), (4, LANES))
        )
        has_rows.append(jnp.broadcast_to(jnp.sum(hit, axis=0, keepdims=True), (4, LANES)))
    inv_idx = jnp.concatenate(inv_rows, axis=0).astype(jnp.int32)
    inv_has = jnp.concatenate(has_rows, axis=0)
    quarter = jnp.right_shift(lax.broadcasted_iota(jnp.int32, (8, LANES), 1), 5)
    nb = nb_ref[...].astype(F32)
    recv_mask = [jnp.where(quarter == k, nb[:, k : k + 1], 0.0) for k in range(4)]

    def copies(slot):
        return [
            pltpu.make_async_remote_copy(
                src_ref=send.at[slot],
                dst_ref=recv.at[slot, k ^ 1],
                send_sem=send_sem.at[slot, k],
                recv_sem=recv_sem.at[slot, k ^ 1],
                device_id=where_to[k],
                device_id_type=MESH,
            )
            for k in range(4)
        ]

    def arrivals(slot):
        return [
            pltpu.make_async_remote_copy(
                src_ref=send.at[slot],
                dst_ref=recv.at[slot, k],
                send_sem=send_sem.at[slot, k],
                recv_sem=recv_sem.at[slot, k],
                device_id=where_to[k],
                device_id_type=MESH,
            )
            for k in range(4)
        ]

    def send_shared(field, slot):
        part = pick_lanes(field[0:8], face_low) * face_mask[0:8]
        part = part + pick_lanes(field[8:16], face_low) * face_mask[8:16]
        send[slot] = part + pltpu.roll(part, 4, 0)
        for k, copy in enumerate(copies(slot)):

            @pl.when(has[k])
            def _():
                copy.start()

    def add_shared(field, slot):
        for k, copy in enumerate(arrivals(slot)):

            @pl.when(has[k])
            def _():
                copy.wait_recv()
                copy.wait_send()

        got = recv[slot, 0] * recv_mask[0]
        for k in range(1, 4):
            got = got + recv[slot, k] * recv_mask[k]
        added = jnp.concatenate(
            [pick_lanes(got, inv_idx[0:8]), pick_lanes(got, inv_idx[8:16])], axis=0
        )
        return field + added * inv_has

    def scatter(rows):
        pieces = []
        for n in range(nodes_el):
            v = rows(n)
            hi, lo = split(jnp.concatenate([v, v], axis=0))
            mask = hmask[n * 16 : (n + 1) * 16, :]
            pieces.append(jnp.concatenate([hi * mask, lo * mask], axis=0))
        res = jnp.dot(
            jnp.concatenate(pieces, axis=1), onehot[...], preferred_element_type=F32
        )
        return res[0:16] + res[16:32]

    row8 = lax.broadcasted_iota(jnp.int32, (8, LANES), 0)
    mass_row = jnp.bitwise_and(row8, 3) == 3
    mass = scatter(lambda n: jnp.where(mass_row, mass_ref[n : n + 1, :], 0.0))
    src_rows = []
    for b in range(blocks):
        src_rows.append(src_ref[:, b * LANES : (b + 1) * LANES])
        src_rows.append(jnp.zeros((1, LANES), F32))
    first = mass + jnp.concatenate(src_rows, axis=0)

    pl.semaphore_wait(
        barrier, has[0].astype(jnp.int32) + has[1].astype(jnp.int32) + writers - 1
    )
    send_shared(first, 0)

    lane_perm = lax.broadcasted_iota(jnp.int32, (LANES, LANES), 1)
    for q in range(points):
        column = rankt_ref[:, q : q + 1]

        def build(j, carry):
            start = pl.multiple_of(j * LANES, LANES)
            perm[q * LANES : (q + 1) * LANES, pl.ds(start, LANES)] = jnp.where(
                column - start == lane_perm, 1.0, 0.0
            ).astype(BF16)
            return carry

        lax.fori_loop(0, perm.shape[1] // LANES, build, 0)
    snaps[...] = jnp.zeros_like(snaps)

    first = add_shared(first, 0)
    axis_row = jnp.bitwise_and(row16, 3) < 3
    source = jnp.where(axis_row, first, 0.0)
    total = jnp.concatenate(
        [jnp.broadcast_to(first[4 * b + 3 : 4 * b + 4, :], (4, LANES)) for b in range(blocks)],
        axis=0,
    )
    half_inverse = jnp.where(axis_row, time_step / total, 0.0)

    low = [jnp.bitwise_and(conn_ref[8 * i : 8 * i + 8, :], LANES - 1) for i in range(3)]
    high = [jnp.right_shift(conn_ref[8 * i : 8 * i + 8, :], 7) for i in range(3)]

    def gradient(u):
        sides = []
        for c in range(3):
            rows = []
            for i in range(3):
                acc = None
                for b in range(blocks):
                    r = 4 * b + c
                    val = pick_lanes(jnp.broadcast_to(u[r : r + 1, :], (8, LANES)), low[i])
                    acc = val if b == 0 else jnp.where(high[i] == b, val, acc)
                rows.append(acc)
            rows.append(jnp.zeros((8, LANES), F32))
            hi, lo = split(jnp.concatenate(rows, axis=0))
            sides.append(jnp.concatenate([hi, lo, hi], axis=0))
        along = jnp.dot(
            w1[...], jnp.concatenate(sides, axis=1), preferred_element_type=F32
        )
        tensor = []
        for c in range(3):
            ref_dir = [
                along[r * points : (r + 1) * points, c * LANES : (c + 1) * LANES]
                for r in range(3)
            ]
            tensor.append(
                [
                    ref_dir[0] * jac_ref[e : e + 1, :]
                    + ref_dir[1] * jac_ref[3 + e : 4 + e, :]
                    + ref_dir[2] * jac_ref[6 + e : 7 + e, :]
                    for e in range(3)
                ]
            )
        return tensor

    def internal_force(t):
        lam = lame_ref[0:1, :]
        mu = lame_ref[1:2, :]
        pressure = lam * (t[0][0] + t[1][1] + t[2][2])
        stress = [[None] * 3 for _ in range(3)]
        for c in range(3):
            for e in range(c, 3):
                s = mu * (t[c][e] + t[e][c])
                if c == e:
                    s = s + pressure
                stress[c][e] = s
                stress[e][c] = s
        weight = pw_ref[...]
        highs = []
        lows = []
        for c in range(3):
            for r in range(3):
                m = stress[c][0] * jac_ref[3 * r : 3 * r + 1, :]
                m = m + stress[c][1] * jac_ref[3 * r + 1 : 3 * r + 2, :]
                m = m + stress[c][2] * jac_ref[3 * r + 2 : 3 * r + 3, :]
                hi, lo = split(m * weight)
                highs.append(hi)
                lows.append(lo)
        side = jnp.concatenate(highs + lows + highs, axis=0)
        values = jnp.dot(w2[...], side, preferred_element_type=F32)
        return scatter(lambda n: values[8 * n : 8 * n + 8, :])

    def record(t, slot_index):
        comps = [
            t[0][0],
            t[1][1],
            t[2][2],
            0.5 * (t[1][2] + t[2][1]),
            0.5 * (t[0][2] + t[2][0]),
            0.5 * (t[0][1] + t[1][0]),
        ]
        for c, value in enumerate(comps):
            start = pl.multiple_of(slot_index * (8 * points) + c * points, points)
            snaps[pl.ds(start, points), :] = value

    velocity = wav_ref[0] * source * half_inverse
    displace = time_step * velocity

    def advance(t, state):
        displace, velocity = state
        slot = lax.rem(t, 2)
        tensor = gradient(displace)
        force = wav_ref[t] * source
        inner = internal_force(tensor)
        send_shared(inner, slot)
        record(tensor, t - 1)
        inner = add_shared(inner, slot)
        velocity = velocity + half_inverse * (force - inner)
        displace = displace + time_step * velocity
        return displace, velocity

    displace, velocity = lax.fori_loop(1, steps, advance, (displace, velocity))
    record(gradient(displace), steps - 1)

    rows_all = steps * 8
    for q in range(points):
        lhs[:, q * LANES : (q + 1) * LANES] = snaps[
            pl.ds(q, rows_all, stride=points), :
        ].astype(BF16)

    def order_for(w):
        start = pl.multiple_of(w * block, block)
        res = jnp.dot(lhs[...], perm[:, pl.ds(start, block)], preferred_element_type=F32)
        return res.reshape(steps, 8, block)[:, 0:6, :].astype(BF16)

    def mine(i):
        return pl.ds(pl.multiple_of(i * block, block), block)

    sends = []
    for i in range(1, writers):
        w = lax.rem(d + i, writers)
        ordered[i] = order_for(w)
        copy = pltpu.make_async_remote_copy(
            src_ref=ordered.at[i],
            dst_ref=out_ref.at[:, :, mine(d)],
            send_sem=out_send_sem.at[i],
            recv_sem=out_recv_sem.at[i],
            device_id=(g, w),
            device_id_type=MESH,
        )
        copy.start()
        sends.append(copy)
    out_ref[:, :, mine(d)] = order_for(d)
    for i in range(1, writers):
        origin = lax.rem(d - i + writers, writers)
        pltpu.make_async_remote_copy(
            src_ref=ordered.at[i],
            dst_ref=out_ref.at[:, :, mine(origin)],
            send_sem=out_send_sem.at[i],
            recv_sem=out_recv_sem.at[i],
            device_id=(g, origin),
            device_id_type=MESH,
        ).wait_recv()
    for copy in sends:
        copy.wait_send()


def solution(mesh):
    groups, writers = mesh.shape["grp"], mesh.shape["dom"]

    def shards(
        connect,
        interface_nodes,
        neighbours,
        point_rank,
        shape_grad,
        inverse_jacobian,
        lame_moduli,
        point_weights,
        mass_elem,
        source_pattern,
        wavelet,
    ):
        nodes_el, elements = connect.shape
        points = point_weights.shape[0]
        point_count = point_rank.shape[1]
        steps = wavelet.shape[0]
        faces = interface_nodes[0]
        facet = faces.reshape(-1, 1)
        facesw = faces[jnp.array([1, 0, 3, 2])].reshape(1, -1)
        conn = jnp.pad(connect, ((0, 24 - nodes_el), (0, 0)))
        rankt = point_rank.reshape(points, elements).T
        w1f = jnp.tile(jnp.pad(shape_grad, ((0, 0), (0, 32 - nodes_el))), (1, 3))
        chan = jnp.arange(8)[:, None] % 4 == jnp.arange(3)[None, :]
        w2f = jnp.where(
            chan[None, :, None, :, None], shape_grad.T[:, None, None, None, :], 0.0
        )
        w2f = jnp.broadcast_to(w2f, (nodes_el, 8, 3, 3, 3 * points))
        w2f = w2f.reshape(nodes_el * 8, 27 * points)
        vmem = pl.BlockSpec(memory_space=pltpu.VMEM)
        smem = pl.BlockSpec(memory_space=pltpu.SMEM)
        return pl.pallas_call(
            functools.partial(kernel, groups, writers, steps, nodes_el),
            out_shape=jax.ShapeDtypeStruct((steps, 6, point_count), BF16),
            in_specs=[vmem] * 13 + [smem],
            out_specs=vmem,
            scratch_shapes=[
                pltpu.VMEM((nodes_el * LANES, LANES), BF16),
                pltpu.VMEM((nodes_el * 16, LANES), BF16),
                pltpu.VMEM((point_count, point_count), BF16),
                pltpu.VMEM(w1f.shape, BF16),
                pltpu.VMEM(w2f.shape, BF16),
                pltpu.VMEM((steps * 8 * points, LANES), F32),
                pltpu.VMEM((steps * 8, point_count), BF16),
                pltpu.VMEM((writers, steps, 6, point_count // writers), BF16),
                pltpu.VMEM((2, 8, LANES), F32),
                pltpu.VMEM((2, 4, 8, LANES), F32),
                pltpu.SemaphoreType.DMA((2, 4)),
                pltpu.SemaphoreType.DMA((2, 4)),
                pltpu.SemaphoreType.DMA((writers,)),
                pltpu.SemaphoreType.DMA((writers,)),
            ],
            compiler_params=pltpu.CompilerParams(
                collective_id=0, has_side_effects=True, vmem_limit_bytes=56 * 1024 * 1024
            ),
            name="window",
        )(
            conn,
            connect.T,
            facet,
            facesw,
            neighbours,
            rankt,
            w1f,
            w2f,
            inverse_jacobian,
            lame_moduli,
            point_weights,
            mass_elem,
            source_pattern,
            wavelet,
        )

    placed = (
        P(None, ("grp", "dom")),
        P(("grp", "dom"), None, None),
        P(("grp", "dom"), None),
        P(("grp", "dom"), None),
        P(),
        P(None, ("grp", "dom")),
        P(None, ("grp", "dom")),
        P(None, ("grp", "dom")),
        P(None, ("grp", "dom")),
        P(None, ("grp", "dom")),
        P(),
    )
    return jax.shard_map(
        shards, mesh=mesh, in_specs=placed, out_specs=P(None, None, ("grp", "dom")), check_vma=False
    )
```

```python
import functools

import jax
import jax.numpy as jnp
from jax import lax
from jax.experimental import pallas as pl
from jax.experimental.pallas import tpu as pltpu
from jax.sharding import PartitionSpec as P

MESH = pl.DeviceIdType.MESH
F32 = jnp.float32
BF16 = jnp.bfloat16
time_step = 0.5
LANES = 128


def split(x):
    hi = x.astype(BF16)
    return hi, (x - hi.astype(F32)).astype(BF16)


def pick_lanes(x, idx):
    return jnp.take_along_axis(x, idx, axis=1, mode="promise_in_bounds")


def kernel(
    groups,
    writers,
    steps,
    nodes_el,
    conn_ref,
    faces_ref,
    nb_ref,
    rank_ref,
    gradt_ref,
    jac_ref,
    lame_ref,
    pw_ref,
    mass_ref,
    src_ref,
    wav_ref,
    out_ref,
    onehot,
    hmask,
    perm,
    w1,
    w2,
    snaps,
    lhs,
    ordered,
    send,
    recv,
    send_sem,
    recv_sem,
    out_send_sem,
    out_recv_sem,
):
    g = lax.axis_index("grp")
    d = lax.axis_index("dom")
    points = pw_ref.shape[0]
    block = out_ref.shape[2] // writers
    blocks = src_ref.shape[1] // LANES

    recv[...] = jnp.zeros_like(recv)
    has = (g > 0, g < groups - 1, d > 0, d < writers - 1)
    where_to = ((g - 1, d), (g + 1, d), (g, d - 1), (g, d + 1))

    barrier = pltpu.get_barrier_semaphore()
    for k in range(2):

        @pl.when(has[k])
        def _():
            pl.semaphore_signal(barrier, inc=1, device_id=where_to[k], device_id_type=MESH)

    for i in range(1, writers):
        pl.semaphore_signal(
            barrier, inc=1, device_id=(g, lax.rem(d + i, writers)), device_id_type=MESH
        )

    lane = lax.broadcasted_iota(jnp.int32, (LANES, LANES), 1)
    row16 = lax.broadcasted_iota(jnp.int32, (16, LANES), 0)
    conn_low = jnp.bitwise_and(conn_ref[...], LANES - 1)
    conn_high = jnp.right_shift(conn_ref[...], 7)
    columns = jnp.concatenate(
        [conn_low.astype(F32), jnp.zeros((LANES - nodes_el, LANES), F32)], axis=0
    ).T
    for n in range(nodes_el):
        hit = jnp.where(columns[:, n : n + 1] == lane.astype(F32), 1.0, 0.0)
        onehot[n * LANES : (n + 1) * LANES, :] = hit.astype(BF16)
        hmask[n * 16 : (n + 1) * 16, :] = jnp.where(
            conn_high[n : n + 1, :] == jnp.right_shift(row16, 2), 1.0, 0.0
        ).astype(BF16)
    gradt = gradt_ref[...]
    depth = 3 * points
    hi = gradt.astype(BF16).astype(F32)
    lo = gradt - hi
    gap = jnp.zeros((32 - nodes_el, depth), F32)
    tall = jnp.concatenate([hi, gap, hi, gap, lo, gap, jnp.zeros((32, depth), F32)], axis=0)
    tall = jnp.concatenate([tall, jnp.zeros((LANES, LANES - depth), F32)], axis=1)
    w1[...] = tall.T[0:depth, 0:96].astype(BF16)
    wide = jnp.concatenate([hi] * 6 + [lo] * 3, axis=1)
    col = lax.broadcasted_iota(jnp.int32, (8, 9 * depth), 1)
    rows = jnp.bitwise_and(lax.broadcasted_iota(jnp.int32, (8, 9 * depth), 0), 3)
    own = (col >= rows * depth) & (col < (rows + 1) * depth)
    for piece in (3, 6):
        own = own | ((col >= (rows + piece) * depth) & (col < (rows + piece + 1) * depth))
    own = own & (rows < 3)
    for n in range(0, nodes_el, 2):
        two = [jnp.where(own, wide[m : m + 1, :], 0.0) for m in (n, n + 1)]
        w2[n * 8 : n * 8 + 16, :] = jnp.concatenate(two, axis=0).astype(BF16)

    faces = faces_ref[0].astype(F32)
    face_row = jnp.concatenate([faces[k : k + 1, :] for k in range(4)], axis=1)
    face_swap = jnp.concatenate([faces[k ^ 1 : (k ^ 1) + 1, :] for k in range(4)], axis=1)
    face_swap = face_swap.astype(jnp.int32)
    face_low = jnp.broadcast_to(jnp.bitwise_and(face_swap, LANES - 1), (8, LANES))
    face_mask = jnp.where(
        jnp.right_shift(face_swap, 7) == jnp.right_shift(row16, 2), 1.0, 0.0
    )
    face_col = jnp.broadcast_to(face_row, (LANES, LANES)).T
    position = lax.broadcasted_iota(jnp.int32, (LANES, LANES), 0).astype(F32)
    inv_rows = []
    has_rows = []
    for b in range(blocks):
        hit = jnp.where(face_col == (lane + b * LANES).astype(F32), 1.0, 0.0)
        inv_rows.append(
            jnp.broadcast_to(jnp.sum(hit * position, axis=0, keepdims=True), (4, LANES))
        )
        has_rows.append(jnp.broadcast_to(jnp.sum(hit, axis=0, keepdims=True), (4, LANES)))
    inv_idx = jnp.concatenate(inv_rows, axis=0).astype(jnp.int32)
    inv_has = jnp.concatenate(has_rows, axis=0)
    quarter = jnp.right_shift(lax.broadcasted_iota(jnp.int32, (8, LANES), 1), 5)
    nb = nb_ref[...].astype(F32)
    recv_mask = [jnp.where(quarter == k, nb[:, k : k + 1], 0.0) for k in range(4)]

    def copies(slot):
        return [
            pltpu.make_async_remote_copy(
                src_ref=send.at[slot],
                dst_ref=recv.at[slot, k ^ 1],
                send_sem=send_sem.at[slot, k],
                recv_sem=recv_sem.at[slot, k ^ 1],
                device_id=where_to[k],
                device_id_type=MESH,
            )
            for k in range(4)
        ]

    def arrivals(slot):
        return [
            pltpu.make_async_remote_copy(
                src_ref=send.at[slot],
                dst_ref=recv.at[slot, k],
                send_sem=send_sem.at[slot, k],
                recv_sem=recv_sem.at[slot, k],
                device_id=where_to[k],
                device_id_type=MESH,
            )
            for k in range(4)
        ]

    def send_shared(field, slot):
        part = pick_lanes(field[0:8], face_low) * face_mask[0:8]
        part = part + pick_lanes(field[8:16], face_low) * face_mask[8:16]
        send[slot] = part + pltpu.roll(part, 4, 0)
        for k, copy in enumerate(copies(slot)):

            @pl.when(has[k])
            def _():
                copy.start()

    def add_shared(field, slot):
        for k, copy in enumerate(arrivals(slot)):

            @pl.when(has[k])
            def _():
                copy.wait_recv()
                copy.wait_send()

        got = recv[slot, 0] * recv_mask[0]
        for k in range(1, 4):
            got = got + recv[slot, k] * recv_mask[k]
        added = jnp.concatenate(
            [pick_lanes(got, inv_idx[0:8]), pick_lanes(got, inv_idx[8:16])], axis=0
        )
        return field + added * inv_has

    def scatter(rows):
        pieces = []
        for n in range(nodes_el):
            v = rows(n)
            hi, lo = split(jnp.concatenate([v, v], axis=0))
            mask = hmask[n * 16 : (n + 1) * 16, :]
            pieces.append(jnp.concatenate([hi * mask, lo * mask], axis=0))
        res = jnp.dot(
            jnp.concatenate(pieces, axis=1), onehot[...], preferred_element_type=F32
        )
        return res[0:16] + res[16:32]

    row8 = lax.broadcasted_iota(jnp.int32, (8, LANES), 0)
    mass_row = jnp.bitwise_and(row8, 3) == 3
    mass = scatter(lambda n: jnp.where(mass_row, mass_ref[n : n + 1, :], 0.0))
    src_rows = []
    for b in range(blocks):
        src_rows.append(src_ref[:, b * LANES : (b + 1) * LANES])
        src_rows.append(jnp.zeros((1, LANES), F32))
    first = mass + jnp.concatenate(src_rows, axis=0)

    pl.semaphore_wait(
        barrier, has[0].astype(jnp.int32) + has[1].astype(jnp.int32) + writers - 1
    )
    send_shared(first, 0)

    rank_row = lax.broadcasted_iota(jnp.int32, (perm.shape[0], LANES), 0)

    def build_order(q):
        start = pl.multiple_of(q * LANES, LANES)
        perm[:, pl.ds(start, LANES)] = jnp.where(
            rank_ref[:, pl.ds(start, LANES)] == rank_row, 1.0, 0.0
        ).astype(BF16)

    for q in range(max(points - steps + 1, 0)):
        build_order(q)

    first = add_shared(first, 0)
    axis_row = jnp.bitwise_and(row16, 3) < 3
    source = jnp.where(axis_row, first, 0.0)
    total = jnp.concatenate(
        [jnp.broadcast_to(first[4 * b + 3 : 4 * b + 4, :], (4, LANES)) for b in range(blocks)],
        axis=0,
    )
    half_inverse = jnp.where(axis_row, time_step / total, 0.0)

    spare = jnp.zeros((24 - nodes_el, LANES), jnp.int32)
    conn_low = jnp.concatenate([conn_low, spare], axis=0)
    conn_high = jnp.concatenate([conn_high, spare], axis=0)
    low = [conn_low[8 * i : 8 * i + 8, :] for i in range(3)]
    high = [conn_high[8 * i : 8 * i + 8, :] for i in range(3)]

    def gradient(u):
        sides = []
        for c in range(3):
            rows = []
            for i in range(3):
                acc = None
                for b in range(blocks):
                    r = 4 * b + c
                    val = pick_lanes(jnp.broadcast_to(u[r : r + 1, :], (8, LANES)), low[i])
                    acc = val if b == 0 else jnp.where(high[i] == b, val, acc)
                rows.append(acc)
            rows.append(jnp.zeros((8, LANES), F32))
            hi, lo = split(jnp.concatenate(rows, axis=0))
            sides.append(jnp.concatenate([hi, lo, hi], axis=0))
        along = jnp.dot(
            w1[...], jnp.concatenate(sides, axis=1), preferred_element_type=F32
        )
        tensor = []
        for c in range(3):
            ref_dir = [
                along[r * points : (r + 1) * points, c * LANES : (c + 1) * LANES]
                for r in range(3)
            ]
            tensor.append(
                [
                    ref_dir[0] * jac_ref[e : e + 1, :]
                    + ref_dir[1] * jac_ref[3 + e : 4 + e, :]
                    + ref_dir[2] * jac_ref[6 + e : 7 + e, :]
                    for e in range(3)
                ]
            )
        return tensor

    def internal_force(t):
        lam = lame_ref[0:1, :]
        mu = lame_ref[1:2, :]
        pressure = lam * (t[0][0] + t[1][1] + t[2][2])
        stress = [[None] * 3 for _ in range(3)]
        for c in range(3):
            for e in range(c, 3):
                s = mu * (t[c][e] + t[e][c])
                if c == e:
                    s = s + pressure
                stress[c][e] = s
                stress[e][c] = s
        weight = pw_ref[...]
        highs = []
        lows = []
        for c in range(3):
            for r in range(3):
                m = stress[c][0] * jac_ref[3 * r : 3 * r + 1, :]
                m = m + stress[c][1] * jac_ref[3 * r + 1 : 3 * r + 2, :]
                m = m + stress[c][2] * jac_ref[3 * r + 2 : 3 * r + 3, :]
                hi, lo = split(m * weight)
                highs.append(hi)
                lows.append(lo)
        side = jnp.concatenate(highs + lows + highs, axis=0)
        values = jnp.dot(w2[...], side, preferred_element_type=F32)
        return scatter(lambda n: values[8 * n : 8 * n + 8, :])

    def record(t, slot_index):
        comps = [
            t[0][0],
            t[1][1],
            t[2][2],
            0.5 * (t[1][2] + t[2][1]),
            0.5 * (t[0][2] + t[2][0]),
            0.5 * (t[0][1] + t[1][0]),
        ]
        for c, value in enumerate(comps):
            start = pl.multiple_of((c * steps + slot_index) * points, points)
            snaps[pl.ds(start, points), :] = value

    velocity = wav_ref[0] * source * half_inverse
    displace = time_step * velocity

    def advance(t, state):
        displace, velocity = state
        slot = lax.rem(t, 2)
        tensor = gradient(displace)
        force = wav_ref[t] * source
        inner = internal_force(tensor)
        send_shared(inner, slot)
        record(tensor, t - 1)
        build_order(t + (points - steps))
        inner = add_shared(inner, slot)
        velocity = velocity + half_inverse * (force - inner)
        displace = displace + time_step * velocity
        return displace, velocity

    displace, velocity = lax.fori_loop(1, steps, advance, (displace, velocity))
    record(gradient(displace), steps - 1)

    rows_all = steps * 6
    for q in range(points):
        lhs[:, q * LANES : (q + 1) * LANES] = snaps[
            pl.ds(q, rows_all, stride=points), :
        ].astype(BF16)

    def order_for(w):
        start = pl.multiple_of(w * block, block)
        res = lax.dot_general(
            lhs[...],
            perm[pl.ds(start, block), :],
            (((1,), (1,)), ((), ())),
            preferred_element_type=F32,
        )
        return res.astype(BF16).reshape(6, steps, block)

    def mine(i):
        return pl.ds(pl.multiple_of(i * block, block), block)

    sends = []
    for i in range(1, writers):
        w = lax.rem(d + i, writers)
        ordered[i] = order_for(w)
        copy = pltpu.make_async_remote_copy(
            src_ref=ordered.at[i],
            dst_ref=out_ref.at[:, :, mine(d)],
            send_sem=out_send_sem.at[i],
            recv_sem=out_recv_sem.at[i],
            device_id=(g, w),
            device_id_type=MESH,
        )
        copy.start()
        sends.append(copy)
    out_ref[:, :, mine(d)] = order_for(d)
    for i in range(1, writers):
        origin = lax.rem(d - i + writers, writers)
        pltpu.make_async_remote_copy(
            src_ref=ordered.at[i],
            dst_ref=out_ref.at[:, :, mine(origin)],
            send_sem=out_send_sem.at[i],
            recv_sem=out_recv_sem.at[i],
            device_id=(g, origin),
            device_id_type=MESH,
        ).wait_recv()
    for copy in sends:
        copy.wait_send()


def solution(mesh):
    groups, writers = mesh.shape["grp"], mesh.shape["dom"]

    def shards(
        connect,
        interface_nodes,
        neighbours,
        point_rank,
        shape_grad,
        inverse_jacobian,
        lame_moduli,
        point_weights,
        mass_elem,
        source_pattern,
        wavelet,
    ):
        nodes_el, elements = connect.shape
        points = point_weights.shape[0]
        point_count = point_rank.shape[1]
        steps = wavelet.shape[0]
        vmem = pl.BlockSpec(memory_space=pltpu.VMEM)
        smem = pl.BlockSpec(memory_space=pltpu.SMEM)
        ordered = pl.pallas_call(
            functools.partial(kernel, groups, writers, steps, nodes_el),
            out_shape=jax.ShapeDtypeStruct((6, steps, point_count), BF16),
            in_specs=[vmem] * 10 + [smem],
            out_specs=vmem,
            scratch_shapes=[
                pltpu.VMEM((nodes_el * LANES, LANES), BF16),
                pltpu.VMEM((nodes_el * 16, LANES), BF16),
                pltpu.VMEM((point_count, point_count), BF16),
                pltpu.VMEM((3 * points, 96), BF16),
                pltpu.VMEM((nodes_el * 8, 27 * points), BF16),
                pltpu.VMEM((steps * 6 * points, LANES), F32),
                pltpu.VMEM((steps * 6, point_count), BF16),
                pltpu.VMEM((writers, 6, steps, point_count // writers), BF16),
                pltpu.VMEM((2, 8, LANES), F32),
                pltpu.VMEM((2, 4, 8, LANES), F32),
                pltpu.SemaphoreType.DMA((2, 4)),
                pltpu.SemaphoreType.DMA((2, 4)),
                pltpu.SemaphoreType.DMA((writers,)),
                pltpu.SemaphoreType.DMA((writers,)),
            ],
            compiler_params=pltpu.CompilerParams(
                collective_id=0, has_side_effects=True, vmem_limit_bytes=56 * 1024 * 1024
            ),
            name="window",
        )(
            connect,
            interface_nodes,
            neighbours,
            point_rank,
            shape_grad.T,
            inverse_jacobian,
            lame_moduli,
            point_weights,
            mass_elem,
            source_pattern,
            wavelet,
        )
        return ordered.transpose(1, 0, 2)

    placed = (
        P(None, ("grp", "dom")),
        P(("grp", "dom"), None, None),
        P(("grp", "dom"), None),
        P(("grp", "dom"), None),
        P(),
        P(None, ("grp", "dom")),
        P(None, ("grp", "dom")),
        P(None, ("grp", "dom")),
        P(None, ("grp", "dom")),
        P(None, ("grp", "dom")),
        P(),
    )
    return jax.shard_map(
        shards, mesh=mesh, in_specs=placed, out_specs=P(None, None, ("grp", "dom")), check_vma=False
    )
```

```python
import functools

import jax
import jax.numpy as jnp
from jax import lax
from jax.experimental import pallas as pl
from jax.experimental.pallas import tpu as pltpu
from jax.sharding import PartitionSpec as P

MESH = pl.DeviceIdType.MESH
F32 = jnp.float32
BF16 = jnp.bfloat16
time_step = 0.5
LANES = 128


def split(x):
    hi = x.astype(BF16)
    return hi, (x - hi.astype(F32)).astype(BF16)


def pick_lanes(x, idx):
    return jnp.take_along_axis(x, idx, axis=1, mode="promise_in_bounds")


def kernel(
    groups,
    writers,
    steps,
    nodes_el,
    conn_ref,
    faces_ref,
    nb_ref,
    rank_ref,
    gradt_ref,
    jac_ref,
    lame_ref,
    pw_ref,
    mass_ref,
    src_ref,
    wav_ref,
    out_ref,
    onehot,
    hmask,
    perm,
    w1,
    w2,
    snaps,
    lhs,
    ordered,
    send,
    recv,
    send_sem,
    recv_sem,
    out_send_sem,
    out_recv_sem,
):
    g = lax.axis_index("grp")
    d = lax.axis_index("dom")
    points = pw_ref.shape[0]
    block = out_ref.shape[2] // writers
    blocks = src_ref.shape[1] // LANES

    recv[...] = jnp.zeros_like(recv)
    has = (g > 0, g < groups - 1, d > 0, d < writers - 1)
    where_to = ((g - 1, d), (g + 1, d), (g, d - 1), (g, d + 1))

    barrier = pltpu.get_barrier_semaphore()
    for k in range(2):

        @pl.when(has[k])
        def _():
            pl.semaphore_signal(barrier, inc=1, device_id=where_to[k], device_id_type=MESH)

    for i in range(1, writers):
        pl.semaphore_signal(
            barrier, inc=1, device_id=(g, lax.rem(d + i, writers)), device_id_type=MESH
        )

    lane = lax.broadcasted_iota(jnp.int32, (LANES, LANES), 1)
    row16 = lax.broadcasted_iota(jnp.int32, (16, LANES), 0)
    faces = faces_ref[0].astype(F32)
    face_row = jnp.concatenate([faces[k : k + 1, :] for k in range(4)], axis=1)
    face_swap = jnp.concatenate([faces[k ^ 1 : (k ^ 1) + 1, :] for k in range(4)], axis=1)
    face_swap = face_swap.astype(jnp.int32)
    face_low = jnp.broadcast_to(jnp.bitwise_and(face_swap, LANES - 1), (8, LANES))
    face_mask = jnp.where(
        jnp.right_shift(face_swap, 7) == jnp.right_shift(row16, 2), 1.0, 0.0
    )
    face_col = jnp.broadcast_to(face_row, (LANES, LANES)).T
    position = lax.broadcasted_iota(jnp.int32, (LANES, LANES), 0).astype(F32)
    inv_rows = []
    has_rows = []
    for b in range(blocks):
        hit = jnp.where(face_col == (lane + b * LANES).astype(F32), 1.0, 0.0)
        inv_rows.append(
            jnp.broadcast_to(jnp.sum(hit * position, axis=0, keepdims=True), (4, LANES))
        )
        has_rows.append(jnp.broadcast_to(jnp.sum(hit, axis=0, keepdims=True), (4, LANES)))
    inv_idx = jnp.concatenate(inv_rows, axis=0).astype(jnp.int32)
    inv_has = jnp.concatenate(has_rows, axis=0)

    conn_low = jnp.bitwise_and(conn_ref[...], LANES - 1)
    conn_high = jnp.right_shift(conn_ref[...], 7)
    columns = jnp.concatenate(
        [conn_low.astype(F32), jnp.zeros((LANES - nodes_el, LANES), F32)], axis=0
    ).T
    for n in range(nodes_el):
        here = jnp.broadcast_to(columns[:, n : n + 1], (LANES, LANES))
        hit = jnp.where(here == lane.astype(F32), 1.0, 0.0)
        onehot[n * LANES : (n + 1) * LANES, 0:LANES] = hit.astype(BF16)
        hit = jnp.where(here == face_low[0:1, :].astype(F32), 1.0, 0.0)
        onehot[n * LANES : (n + 1) * LANES, LANES:] = hit.astype(BF16)
        hmask[n * 16 : (n + 1) * 16, :] = jnp.where(
            conn_high[n : n + 1, :] == jnp.right_shift(row16, 2), 1.0, 0.0
        ).astype(BF16)
    gradt = gradt_ref[...]
    depth = 3 * points
    hi = gradt.astype(BF16).astype(F32)
    lo = gradt - hi
    gap = jnp.zeros((32 - nodes_el, depth), F32)
    tall = jnp.concatenate([hi, gap, hi, gap, lo, gap, jnp.zeros((32, depth), F32)], axis=0)
    tall = jnp.concatenate([tall, jnp.zeros((LANES, LANES - depth), F32)], axis=1)
    w1[...] = tall.T[0:depth, 0:96].astype(BF16)
    wide = jnp.concatenate([hi] * 6 + [lo] * 3, axis=1)
    col = lax.broadcasted_iota(jnp.int32, (8, 9 * depth), 1)
    rows = jnp.bitwise_and(lax.broadcasted_iota(jnp.int32, (8, 9 * depth), 0), 3)
    own = (col >= rows * depth) & (col < (rows + 1) * depth)
    for piece in (3, 6):
        own = own | ((col >= (rows + piece) * depth) & (col < (rows + piece + 1) * depth))
    own = own & (rows < 3)
    for n in range(0, nodes_el, 2):
        two = [jnp.where(own, wide[m : m + 1, :], 0.0) for m in (n, n + 1)]
        w2[n * 8 : n * 8 + 16, :] = jnp.concatenate(two, axis=0).astype(BF16)

    quarter = jnp.right_shift(lax.broadcasted_iota(jnp.int32, (8, LANES), 1), 5)
    nb = nb_ref[...].astype(F32)
    recv_mask = [jnp.where(quarter == k, nb[:, k : k + 1], 0.0) for k in range(4)]

    def copies(slot):
        return [
            pltpu.make_async_remote_copy(
                src_ref=send.at[slot],
                dst_ref=recv.at[slot, k ^ 1],
                send_sem=send_sem.at[slot, k],
                recv_sem=recv_sem.at[slot, k ^ 1],
                device_id=where_to[k],
                device_id_type=MESH,
            )
            for k in range(4)
        ]

    def arrivals(slot):
        return [
            pltpu.make_async_remote_copy(
                src_ref=send.at[slot],
                dst_ref=recv.at[slot, k],
                send_sem=send_sem.at[slot, k],
                recv_sem=recv_sem.at[slot, k],
                device_id=where_to[k],
                device_id_type=MESH,
            )
            for k in range(4)
        ]

    def send_shared(field, slot):
        part = field[:, LANES:] * face_mask
        part = part[0:8] + part[8:16]
        send[slot] = part + pltpu.roll(part, 4, 0)
        for k, copy in enumerate(copies(slot)):

            @pl.when(has[k])
            def _():
                copy.start()

    def shared_sum(slot):
        for k, copy in enumerate(arrivals(slot)):

            @pl.when(has[k])
            def _():
                copy.wait_recv()
                copy.wait_send()

        got = recv[slot, 0] * recv_mask[0]
        for k in range(1, 4):
            got = got + recv[slot, k] * recv_mask[k]
        return got

    def at_nodes(got):
        added = jnp.concatenate(
            [pick_lanes(got, inv_idx[0:8]), pick_lanes(got, inv_idx[8:16])], axis=0
        )
        return added * inv_has

    def scatter(rows):
        pieces = []
        for n in range(nodes_el):
            v = rows(n)
            hi, lo = split(jnp.concatenate([v, v], axis=0))
            mask = hmask[n * 16 : (n + 1) * 16, :]
            pieces.append(jnp.concatenate([hi * mask, lo * mask], axis=0))
        res = jnp.dot(
            jnp.concatenate(pieces, axis=1), onehot[...], preferred_element_type=F32
        )
        return res[0:16] + res[16:32]

    row8 = lax.broadcasted_iota(jnp.int32, (8, LANES), 0)
    mass_row = jnp.bitwise_and(row8, 3) == 3
    mass = scatter(lambda n: jnp.where(mass_row, mass_ref[n : n + 1, :], 0.0))
    src_rows = []
    for b in range(blocks):
        src_rows.append(src_ref[:, b * LANES : (b + 1) * LANES])
        src_rows.append(jnp.zeros((1, LANES), F32))
    source_rows = jnp.concatenate(src_rows, axis=0)
    source_low = jnp.concatenate(
        [pick_lanes(source_rows[i : i + 8], face_low) for i in (0, 8)], axis=0
    )
    first = mass + jnp.concatenate([source_rows, source_low], axis=1)

    pl.semaphore_wait(
        barrier, has[0].astype(jnp.int32) + has[1].astype(jnp.int32) + writers - 1
    )
    send_shared(first, 0)

    rank_row = lax.broadcasted_iota(jnp.int32, (perm.shape[0], LANES), 0)

    def build_order(q):
        start = pl.multiple_of(q * LANES, LANES)
        perm[:, pl.ds(start, LANES)] = jnp.where(
            rank_ref[:, pl.ds(start, LANES)] == rank_row, 1.0, 0.0
        ).astype(BF16)

    half = steps // 2
    tables = -(-points // half)
    for q in range(min(tables, points)):
        build_order(q)

    first = first[:, 0:LANES] + at_nodes(shared_sum(0))
    axis_row = jnp.bitwise_and(row16, 3) < 3
    source = jnp.where(axis_row, first, 0.0)
    total = jnp.concatenate(
        [jnp.broadcast_to(first[4 * b + 3 : 4 * b + 4, :], (4, LANES)) for b in range(blocks)],
        axis=0,
    )
    half_inverse = jnp.where(axis_row, time_step / total, 0.0)

    spare = jnp.zeros((24 - nodes_el, LANES), jnp.int32)
    conn_low = jnp.concatenate([conn_low, spare], axis=0)
    conn_high = jnp.concatenate([conn_high, spare], axis=0)
    low = [conn_low[8 * i : 8 * i + 8, :] for i in range(3)]
    high = [conn_high[8 * i : 8 * i + 8, :] for i in range(3)]

    def at_elements(rows_of):
        out = []
        for i in range(3):
            acc = None
            for b in range(blocks):
                val = pick_lanes(jnp.broadcast_to(rows_of(b), (8, LANES)), low[i])
                acc = val if b == 0 else jnp.where(high[i] == b, val, acc)
            out.append(acc)
        return out

    inv_f = inv_idx.astype(F32)
    place = [x.astype(jnp.int32) for x in at_elements(lambda b: inv_f[4 * b : 4 * b + 1, :])]
    coef = (-time_step) * half_inverse * inv_has
    coef = at_elements(lambda b: coef[4 * b : 4 * b + 1, :])

    def gather(u):
        return tuple(
            tuple(at_elements(lambda b: u[4 * b + c : 4 * b + c + 1, :])) for c in range(3)
        )

    def corrected(values, got):
        out = []
        for c in range(3):
            row = jnp.broadcast_to(got[c : c + 1, :], (8, LANES))
            out.append(
                tuple(values[c][i] + pick_lanes(row, place[i]) * coef[i] for i in range(3))
            )
        return tuple(out)

    def gradient(values):
        sides = []
        for c in range(3):
            rows = list(values[c]) + [jnp.zeros((8, LANES), F32)]
            hi, lo = split(jnp.concatenate(rows, axis=0))
            sides.append(jnp.concatenate([hi, lo, hi], axis=0))
        along = jnp.dot(
            w1[...], jnp.concatenate(sides, axis=1), preferred_element_type=F32
        )
        tensor = []
        for c in range(3):
            ref_dir = [
                along[r * points : (r + 1) * points, c * LANES : (c + 1) * LANES]
                for r in range(3)
            ]
            tensor.append(
                [
                    ref_dir[0] * jac_ref[e : e + 1, :]
                    + ref_dir[1] * jac_ref[3 + e : 4 + e, :]
                    + ref_dir[2] * jac_ref[6 + e : 7 + e, :]
                    for e in range(3)
                ]
            )
        return tensor

    def internal_force(t):
        lam = lame_ref[0:1, :]
        mu = lame_ref[1:2, :]
        pressure = lam * (t[0][0] + t[1][1] + t[2][2])
        stress = [[None] * 3 for _ in range(3)]
        for c in range(3):
            for e in range(c, 3):
                s = mu * (t[c][e] + t[e][c])
                if c == e:
                    s = s + pressure
                stress[c][e] = s
                stress[e][c] = s
        weight = pw_ref[...]
        highs = []
        lows = []
        for c in range(3):
            for r in range(3):
                m = stress[c][0] * jac_ref[3 * r : 3 * r + 1, :]
                m = m + stress[c][1] * jac_ref[3 * r + 1 : 3 * r + 2, :]
                m = m + stress[c][2] * jac_ref[3 * r + 2 : 3 * r + 3, :]
                hi, lo = split(m * weight)
                highs.append(hi)
                lows.append(lo)
        side = jnp.concatenate(highs + lows + highs, axis=0)
        values = jnp.dot(w2[...], side, preferred_element_type=F32)
        return scatter(lambda n: values[8 * n : 8 * n + 8, :])

    def record(t, slot_index):
        comps = [
            t[0][0],
            t[1][1],
            t[2][2],
            0.5 * (t[1][2] + t[2][1]),
            0.5 * (t[0][2] + t[2][0]),
            0.5 * (t[0][1] + t[1][0]),
        ]
        for c, value in enumerate(comps):
            start = (slot_index // half) * 6 + c
            start = pl.multiple_of((start * half + lax.rem(slot_index, half)) * points, points)
            snaps[pl.ds(start, points), :] = value

    velocity = wav_ref[0] * source * half_inverse
    displace = time_step * velocity

    def order_for(w):
        start = pl.multiple_of(w * block, block)
        res = lax.dot_general(
            lhs[...],
            perm[pl.ds(start, block), :],
            (((1,), (1,)), ((), ())),
            preferred_element_type=F32,
        )
        return res.astype(BF16).reshape(6, half, block)

    def mine(i):
        return pl.ds(pl.multiple_of(i * block, block), block)

    def parcel(h, i, column, target):
        return pltpu.make_async_remote_copy(
            src_ref=ordered.at[h, i],
            dst_ref=out_ref.at[:, h * half : (h + 1) * half, mine(column)],
            send_sem=out_send_sem.at[h, i],
            recv_sem=out_recv_sem.at[h, i],
            device_id=(g, target),
            device_id_type=MESH,
        )

    def ship(h):
        count = 6 * half
        for q in range(points):
            lhs[:, q * LANES : (q + 1) * LANES] = snaps[
                pl.ds(h * count * points + q, count, stride=points), :
            ].astype(BF16)
        for i in range(1, writers):
            w = lax.rem(d + i, writers)
            ordered[h, i] = order_for(w)
            parcel(h, i, d, w).start()
        out_ref[:, h * half : (h + 1) * half, mine(d)] = order_for(d)

    def advance(t, state, extra):
        values, displace, velocity = state
        slot = lax.rem(t, 2)
        tensor = gradient(values)
        inner = internal_force(tensor)
        send_shared(inner, slot)
        velocity = velocity + half_inverse * (wav_ref[t] * source - inner[:, 0:LANES])
        displace = displace + time_step * velocity
        values = gather(displace)
        record(tensor, t - 1)
        extra(t)
        got = shared_sum(slot)
        values = corrected(values, got)
        change = half_inverse * at_nodes(got)
        return values, displace - time_step * change, velocity - change

    def early(t, state):
        def extra(t):
            for i in range(tables):
                build_order(jnp.minimum(t * tables + i, points - 1))

        return advance(t, state, extra)

    state = (gather(displace), displace, velocity)
    state = lax.fori_loop(1, half, early, state)
    state = advance(jnp.int32(half), state, lambda t: ship(0))
    state = lax.fori_loop(
        half + 1, steps, lambda t, held: advance(t, held, lambda t: None), state
    )
    record(gradient(state[0]), jnp.int32(steps - 1))
    ship(1)
    for h in range(2):
        for i in range(1, writers):
            origin = lax.rem(d - i + writers, writers)
            parcel(h, i, origin, origin).wait_recv()
            w = lax.rem(d + i, writers)
            parcel(h, i, d, w).wait_send()


def solution(mesh):
    groups, writers = mesh.shape["grp"], mesh.shape["dom"]

    def shards(
        connect,
        interface_nodes,
        neighbours,
        point_rank,
        shape_grad,
        inverse_jacobian,
        lame_moduli,
        point_weights,
        mass_elem,
        source_pattern,
        wavelet,
    ):
        nodes_el, elements = connect.shape
        points = point_weights.shape[0]
        point_count = point_rank.shape[1]
        steps = wavelet.shape[0]
        vmem = pl.BlockSpec(memory_space=pltpu.VMEM)
        smem = pl.BlockSpec(memory_space=pltpu.SMEM)
        ordered = pl.pallas_call(
            functools.partial(kernel, groups, writers, steps, nodes_el),
            out_shape=jax.ShapeDtypeStruct((6, steps, point_count), BF16),
            in_specs=[vmem] * 10 + [smem],
            out_specs=vmem,
            scratch_shapes=[
                pltpu.VMEM((nodes_el * LANES, 2 * LANES), BF16),
                pltpu.VMEM((nodes_el * 16, LANES), BF16),
                pltpu.VMEM((point_count, point_count), BF16),
                pltpu.VMEM((3 * points, 96), BF16),
                pltpu.VMEM((nodes_el * 8, 27 * points), BF16),
                pltpu.VMEM((steps * 6 * points, LANES), F32),
                pltpu.VMEM((steps // 2 * 6, point_count), BF16),
                pltpu.VMEM((2, writers, 6, steps // 2, point_count // writers), BF16),
                pltpu.VMEM((2, 8, LANES), F32),
                pltpu.VMEM((2, 4, 8, LANES), F32),
                pltpu.SemaphoreType.DMA((2, 4)),
                pltpu.SemaphoreType.DMA((2, 4)),
                pltpu.SemaphoreType.DMA((2, writers)),
                pltpu.SemaphoreType.DMA((2, writers)),
            ],
            compiler_params=pltpu.CompilerParams(
                collective_id=0, has_side_effects=True, vmem_limit_bytes=56 * 1024 * 1024
            ),
            name="window",
        )(
            connect,
            interface_nodes,
            neighbours,
            point_rank,
            shape_grad.T,
            inverse_jacobian,
            lame_moduli,
            point_weights,
            mass_elem,
            source_pattern,
            wavelet,
        )
        return ordered.transpose(1, 0, 2)

    placed = (
        P(None, ("grp", "dom")),
        P(("grp", "dom"), None, None),
        P(("grp", "dom"), None),
        P(("grp", "dom"), None),
        P(),
        P(None, ("grp", "dom")),
        P(None, ("grp", "dom")),
        P(None, ("grp", "dom")),
        P(None, ("grp", "dom")),
        P(None, ("grp", "dom")),
        P(),
    )
    return jax.shard_map(
        shards, mesh=mesh, in_specs=placed, out_specs=P(None, None, ("grp", "dom")), check_vma=False
    )
```
